32 devices in a mesh: day: 8 (over y, x, core), year: 4 (over z).
Axes of the slice: x: 2, y: 2, z: 4, core: 2. Of those that a mesh axis runs over, the one named last changes fastest.
Arguments:
- field: bfloat16 [16, 184, 2, 11520], P('year', 'day'), may hold values from -14 to 14
- day_index: int32 [16, 184], P('year', 'day'), may hold values from 0 to 183, as said below
- sample_count: int32 [16, 184, 2], P('year', 'day'), may hold values from 1 to 4
Outputs:
- anomaly: bfloat16 [16, 184, 2, 11520], P('year', 'day')
- climatology: bfloat16 [184, 2, 11520], P('day', None, 'year')
The draws below stay inside these ranges and needn't reach their ends.
Inputs may be any that keep to these rules, and one draw needn't show every extreme that they name: In each year either day_index[y, s] = s for every slot, or there is a slot from which on day_index[y, s] = (s + 1) mod 184 and before which day_index[y, s] = s.
All inputs are finite; a program needn't handle non-finite values.
Results may differ from the reference program's by a relative error of at most 0.001.
Values sent between devices are 32-bit elements; how exact they have to be, the bound alone decides.
No kernel may reach another device: no remote copies, remote signals or barrier semaphores. Data moves between devices by JAX's collectives and lax.ppermute only.
A program may use at most 128 MiB of HBM per device.

```python
import math
import jax
import jax.numpy as jnp
from jax import lax

HOURS = 2
HALF = 30
DAYS = 184
YEARS = 16
CELLS = 11520


def calendar(key):
    inner = jax.random.fold_in(key, 11)
    first_key, second_key = jax.random.split(inner)
    leap_flag = jax.random.randint(first_key, (YEARS,), 0, 2)
    cut_slot = jax.random.randint(second_key, (YEARS,), 0, DAYS)
    slots = jnp.arange(DAYS, dtype=jnp.int32)[None, :]
    moved = (slots >= cut_slot[:, None]).astype(jnp.int32) * (1 - leap_flag[:, None])
    return jnp.mod(slots + moved, DAYS).astype(jnp.int32)


def draw_day_index(key, part):
    return calendar(key)


def draw_field(key, part):
    calendar_days = calendar(key)
    inner = jax.random.fold_in(key, 23)
    keys = jax.random.split(inner, 4)
    phase = jax.random.uniform(keys[0], (CELLS,), jnp.float32, 0.0, 2.0 * math.pi)
    amplitude = jax.random.uniform(keys[1], (HOURS, CELLS), jnp.float32, 1.0, 3.0)
    day_axis = jnp.arange(DAYS, dtype=jnp.float32)[:, None, None]
    season = amplitude[None] * jnp.cos(2.0 * math.pi * day_axis / DAYS + phase[None, None, :])
    rough = 0.8 * jnp.clip(jax.random.normal(keys[2], (DAYS, HOURS, CELLS), jnp.float32), -3.0, 3.0)
    base_field = season + rough
    noise = jnp.clip(jax.random.normal(keys[3], (YEARS, DAYS, HOURS, CELLS), jnp.float32), -4.0, 4.0)
    values = base_field[calendar_days] + noise
    return values.astype(jnp.bfloat16)


def place_ends(result, stream_key, low, largest):
    index_at = [jax.random.randint(jax.random.fold_in(stream_key, axis), (), 0, length) for axis, length in enumerate(result.shape)]
    longest = result.shape.index(max(result.shape))
    beside = index_at[:longest] + [(index_at[longest] + 1) % result.shape[longest]] + index_at[longest + 1:]
    return result.at[tuple(index_at)].set(low).at[tuple(beside)].set(largest)


def setup_inputs(seed: int = 0) -> dict:
    seeds = jax.random.split(jax.random.key(seed), 4)
    return {
        "field": draw_field(jax.random.fold_in(seeds[3], 71), 0),
        "day_index": draw_day_index(jax.random.fold_in(seeds[3], 71), 0),
        "sample_count": place_ends(jax.random.randint(seeds[2], (YEARS, DAYS, HOURS), 1, 5), jax.random.fold_in(seeds[2], 1), 1, 4).astype(jnp.int32),
    }


def reference(field, day_index, sample_count):
    weights = sample_count.astype(jnp.float32)

    def add_year(carry, inputs):
        rows, days, counts = inputs
        values = rows.astype(jnp.float32) * counts[:, :, None]
        sums = carry[0] + jax.ops.segment_sum(values, days, num_segments=DAYS)
        totals = carry[1] + jax.ops.segment_sum(counts, days, num_segments=DAYS)
        return (sums, totals), None

    initial = (jnp.zeros((DAYS, HOURS, CELLS), jnp.float32), jnp.zeros((DAYS, HOURS), jnp.float32))
    (day_sums, day_counts), _ = lax.scan(add_year, initial, (field, day_index, weights))
    window_sums = jnp.zeros((DAYS, HOURS, CELLS), jnp.float32)
    window_counts = jnp.zeros((DAYS, HOURS), jnp.float32)
    for offset in range(-HALF, HALF + 1):
        window_sums = window_sums + jnp.roll(day_sums, -offset, axis=0)
        window_counts = window_counts + jnp.roll(day_counts, -offset, axis=0)
    climate = window_sums / window_counts[:, :, None]

    def anomaly_year(inputs):
        rows, days = inputs
        return (rows.astype(jnp.float32) - climate[days]).astype(jnp.bfloat16)

    anomaly = lax.map(anomaly_year, (field, day_index))
    return anomaly, climate.astype(jnp.bfloat16)
```

```python
import jax
import jax.numpy as jnp
from jax import lax
from jax.experimental import pallas as pl
from jax.experimental.pallas import tpu as pltpu
from jax.sharding import PartitionSpec as P

HALF = 30
LANE = 128
CHUNKS = 2
VMEM = 60 * 1024 * 1024


def params():
    return pltpu.CompilerParams(vmem_limit_bytes=VMEM)


def vmem():
    return pl.BlockSpec(memory_space=pltpu.VMEM)


def anywhere():
    return pl.BlockSpec(memory_space=pl.ANY)


def widths(cells, shares):
    tiles = -(-cells // LANE)
    per_share = -(-tiles // shares)
    sizes = [per_share // CHUNKS + (index >= CHUNKS - per_share % CHUNKS) for index in range(CHUNKS)]
    starts = [shares * LANE * sum(sizes[:index]) for index in range(CHUNKS)]
    return [size * LANE for size in sizes], starts


def span(start, width, share, cells):
    low = start + share * width
    return low, max(0, min(width, cells - low))


def two_terms(value):
    high = value.astype(jnp.bfloat16)
    rest = value - high.astype(jnp.float32)
    return high, rest.astype(jnp.bfloat16)


def partial_sums(field, selector, width, start, shares, with_counts):
    year_dev, day_dev, hours, cells = field.shape
    rows, slots = selector.shape
    full = width + (LANE if with_counts else 0)
    spans = [span(start, width, share, cells) for share in range(shares)]

    def kernel(field_ref, selector_ref, out_ref, held, sems):
        def copy(share):
            low, size = spans[share]
            return pltpu.make_async_copy(
                field_ref.at[:, :, :, pl.ds(low, size)],
                held.at[share, :, :, :, pl.ds(0, size)],
                sems.at[share],
            )

        for share in range(shares):
            if spans[share][1]:
                copy(share).start()
        chosen = selector_ref[...]
        if with_counts:
            counts = jnp.dot(
                chosen, jnp.ones((slots, LANE), jnp.bfloat16), preferred_element_type=jnp.float32
            )
        for share in range(shares):
            size = spans[share][1]
            if size:
                copy(share).wait()
                values = held[share, :, :, :, :size].reshape(slots, size)
                out_ref[share, :, :size] = jnp.dot(
                    chosen, values, preferred_element_type=jnp.float32
                )
            if size < width:
                out_ref[share, :, size:width] = jnp.zeros((rows, width - size), jnp.float32)
            if with_counts:
                out_ref[share, :, width:] = counts

    return pl.pallas_call(
        kernel,
        in_specs=[anywhere(), vmem()],
        out_specs=vmem(),
        out_shape=jax.ShapeDtypeStruct((shares, rows, full), jnp.float32),
        scratch_shapes=[
            pltpu.VMEM((shares, year_dev, day_dev, hours, width), jnp.bfloat16),
            pltpu.SemaphoreType.DMA((shares,)),
        ],
        compiler_params=params(),
        cost_estimate=pl.CostEstimate(
            flops=2 * rows * slots * full * shares, bytes_accessed=slots * cells, transcendentals=0
        ),
        name="partial_sums",
    )(field, selector)


def smoothed(pieces, bands, counts, width):
    rows, full = bands[0].shape[0], pieces[0].shape[1]
    with_counts = counts is None
    amount = len(pieces)

    def kernel(*refs):
        piece_refs, band_refs, rest = refs[:amount], refs[amount : 2 * amount], refs[2 * amount :]
        total = jnp.zeros((rows, full), jnp.float32)
        for piece_ref, band_ref in zip(piece_refs, band_refs):
            band = band_ref[...]
            for term in two_terms(piece_ref[...]):
                total += jnp.dot(band, term, preferred_element_type=jnp.float32)
        if with_counts:
            window_counts = total[:, width : width + 1]
            rest[1][...] = total[:, width:]
            rest[0][...] = total[:, :width] / window_counts
        else:
            rest[1][...] = total / rest[0][:, :1]

    out_shape = jax.ShapeDtypeStruct((rows, width), jnp.float32)
    operands = list(pieces) + list(bands)
    if with_counts:
        out_shape = (out_shape, jax.ShapeDtypeStruct((rows, LANE), jnp.float32))
        out_specs = (vmem(), vmem())
    else:
        operands.append(counts)
        out_specs = vmem()
    return pl.pallas_call(
        kernel,
        in_specs=[vmem()] * len(operands),
        out_specs=out_specs,
        out_shape=out_shape,
        compiler_params=params(),
        cost_estimate=pl.CostEstimate(
            flops=2 * rows * 4 * rows * full, bytes_accessed=4 * rows * full, transcendentals=0
        ),
        name="smoothed",
    )(*operands)


def anomalies(field, picker, place, own, streams, width, start, shares, previous):
    year_dev, day_dev, hours, cells = field.shape
    slots, rows = picker.shape
    spans = [span(start, width, share, cells) for share in range(shares)]
    flat = [own] + list(streams[0]) + list(streams[1])
    steps = shares - 1

    def kernel(place_ref, field_ref, picker_ref, *refs):
        arrived = refs[: len(flat)]
        refs = refs[len(flat) :]
        if previous is not None:
            refs = refs[1:]
        out_ref, climate_ref, held, made, chosen, in_sems, out_sems = refs
        where, turned = place_ref[0], place_ref[1]

        def load(share):
            low, size = spans[share]
            return pltpu.make_async_copy(
                field_ref.at[:, :, :, pl.ds(low, size)],
                held.at[share, :, :, :, pl.ds(0, size)],
                in_sems.at[share],
            )

        def store(share):
            low, size = spans[share]
            return pltpu.make_async_copy(
                made.at[share, :, :, :, pl.ds(0, size)],
                out_ref.at[:, :, :, pl.ds(low, size)],
                out_sems.at[share],
            )

        for share in range(shares):
            if spans[share][1]:
                load(share).start()
        pick = picker_ref[...]
        for share in range(shares):
            size = spans[share][1]

            for device in range(shares):
                if device == share:
                    @pl.when(where == device)
                    def _():
                        chosen[...] = arrived[0][...]
                else:
                    step = abs(device - share)
                    for flip in range(2):
                        stream = flip if device > share else 1 - flip

                        @pl.when((where == device) & (turned == flip))
                        def _():
                            chosen[...] = arrived[1 + stream * steps + step - 1][...]

            climate = chosen[...]
            climate_ref[:, share * width : (share + 1) * width] = climate.astype(jnp.bfloat16)
            if size:
                climate = climate[:, :size]
                high = climate.astype(jnp.bfloat16)
                rest = climate - high.astype(jnp.float32)
                middle = rest.astype(jnp.bfloat16)
                low_part = (rest - middle.astype(jnp.float32)).astype(jnp.bfloat16)
                expected = jnp.dot(pick, high, preferred_element_type=jnp.float32)
                expected += jnp.dot(pick, middle, preferred_element_type=jnp.float32) + jnp.dot(
                    pick, low_part, preferred_element_type=jnp.float32
                )
                load(share).wait()
                values = held[share, :, :, :, :size].reshape(slots, size).astype(jnp.float32)
                made[share, :, :, :, :size] = (
                    (values - expected).astype(jnp.bfloat16).reshape(year_dev, day_dev, hours, size)
                )
                store(share).start()
        for share in range(shares):
            if spans[share][1]:
                store(share).wait()

    operands = [place, field, picker] + flat
    specs = [pl.BlockSpec(memory_space=pltpu.SMEM), anywhere(), vmem()] + [vmem()] * len(flat)
    aliases = {}
    if previous is not None:
        aliases = {len(operands): 0}
        operands.append(previous)
        specs.append(anywhere())
    return pl.pallas_call(
        kernel,
        in_specs=specs,
        out_specs=(anywhere(), vmem()),
        out_shape=(
            jax.ShapeDtypeStruct(field.shape, jnp.bfloat16),
            jax.ShapeDtypeStruct((rows, shares * width), jnp.bfloat16),
        ),
        scratch_shapes=[
            pltpu.VMEM((shares, year_dev, day_dev, hours, width), jnp.bfloat16),
            pltpu.VMEM((shares, year_dev, day_dev, hours, width), jnp.bfloat16),
            pltpu.VMEM((rows, width), jnp.float32),
            pltpu.SemaphoreType.DMA((shares,)),
            pltpu.SemaphoreType.DMA((shares,)),
        ],
        input_output_aliases=aliases,
        compiler_params=params(),
        cost_estimate=pl.CostEstimate(
            flops=6 * rows * slots * width * shares,
            bytes_accessed=4 * slots * width * shares,
            transcendentals=0,
        ),
        name="anomalies",
    )(*operands)


def lanes(days, shares, turn):
    pairs = []
    for day in range(days):
        for share in range(shares):
            ahead = share + (1 if day % 2 == turn else -1)
            if 0 <= ahead < shares:
                pairs.append((day * shares + share, day * shares + ahead))
            elif (day ^ 1) < days:
                pairs.append((day * shares + share, (day ^ 1) * shares + share))
    return pairs


def build():
    def local(field, day_index, sample_count):
        year_dev, day_dev, hours, cells = field.shape
        days = lax.axis_size("day")
        shares = lax.axis_size("year")
        n_days = day_dev * days
        rows_days = day_dev + 1
        rows = rows_days * hours
        slots = year_dev * day_dev * hours
        day = lax.axis_index("day")
        share = lax.axis_index("year")
        parity = lax.rem(day, 2)
        chunk_widths, chunk_starts = widths(cells, shares)
        hops = [lanes(days, shares, turn) for turn in range(2)]
        rising = [parity == 0, parity == 1]
        positions = [jnp.where(up, share, shares - 1 - share) for up in rising]

        offsets = jnp.mod(day_index - day * day_dev, n_days)
        offsets = jnp.broadcast_to(offsets[:, :, None], (year_dev, day_dev, hours)).reshape(1, slots)
        counts = sample_count.reshape(1, slots)
        row = lax.broadcasted_iota(jnp.int32, (rows, slots), 0)
        column = lax.broadcasted_iota(jnp.int32, (rows, slots), 1)
        match = (row // hours == offsets) & (lax.rem(row, hours) == lax.rem(column, hours))
        selector = jnp.where(match, counts, 0).astype(jnp.bfloat16)
        picker = jnp.transpose(match.astype(jnp.bfloat16))

        def send(value, pairs, axes=("day", "year")):
            return lax.ppermute(value, axes, pairs)

        partials = [
            partial_sums(field, selector, chunk_widths[k], chunk_starts[k], shares, k == 0)
            for k in range(CHUNKS)
        ]
        received = [[None, None] for _ in range(CHUNKS)]
        for step in range(1, shares):
            for k in range(CHUNKS):
                for s in range(2):
                    ahead = jnp.minimum(shares - step + positions[s], shares - 1)
                    index = jnp.where(rising[s], ahead, shares - 1 - ahead)
                    value = lax.dynamic_index_in_dim(partials[k], index, 0, False)
                    if received[k][s] is not None:
                        value = value + jnp.where(positions[s] > 0, received[k][s], 0.0)
                    received[k][s] = send(value, hops[s])
        climates = []
        window_counts = None
        for k in range(CHUNKS):
            total = lax.dynamic_index_in_dim(partials[k], share, 0, False)
            for s in range(2):
                if received[k][s] is not None:
                    total = total + jnp.where(positions[s] > 0, received[k][s], 0.0)
            pieces, bands = [], []
            reach = -(-(HALF + day_dev) // day_dev)
            for distance in range(-reach, reach + 1):
                kept = [
                    r
                    for r in range(rows_days)
                    if any(abs(distance * day_dev + r - j) <= HALF for j in range(rows_days))
                ]
                if not kept:
                    continue
                low = kept[0]
                high = kept[-1] + 1
                if distance == 0:
                    piece = total
                else:
                    piece = total[low * hours : high * hours]
                    pairs = [(source, (source - distance) % days) for source in range(days)]
                    piece = send(piece, pairs, "day")
                target = lax.broadcasted_iota(jnp.int32, (rows, (high - low) * hours), 0)
                source = lax.broadcasted_iota(jnp.int32, (rows, (high - low) * hours), 1)
                apart = distance * day_dev + low + source // hours - target // hours
                same = lax.rem(source, hours) == lax.rem(target, hours)
                pieces.append(piece)
                bands.append((same & (jnp.abs(apart) <= HALF)).astype(jnp.bfloat16))
            if k == 0:
                climate, window_counts = smoothed(pieces, bands, None, chunk_widths[k])
            else:
                climate = smoothed(pieces, bands, window_counts, chunk_widths[k])
            climates.append(climate)
        gathered = [[[], []] for _ in range(CHUNKS)]
        for _ in range(1, shares):
            for k in range(CHUNKS):
                for s in range(2):
                    value = gathered[k][s][-1] if gathered[k][s] else climates[k]
                    gathered[k][s].append(send(value, hops[s]))
        place = jnp.stack([share, parity]).astype(jnp.int32)
        anomaly, parts = None, []
        for k in range(CHUNKS):
            anomaly, part = anomalies(
                field, picker, place, climates[k], gathered[k], chunk_widths[k], chunk_starts[k],
                shares, anomaly,
            )
            parts.append(part)
        whole = jnp.concatenate(parts, axis=1)
        share_width = cells // shares
        mine = lax.dynamic_slice_in_dim(whole, share * share_width, share_width, 1)
        mine = mine.reshape(rows_days, hours, share_width)[:day_dev]
        return anomaly, mine

    return local


def solution(mesh):
    return jax.shard_map(
        build(),
        mesh=mesh,
        in_specs=(P("year", "day", None, None), P("year", "day"), P("year", "day", None)),
        out_specs=(P("year", "day", None, None), P("day", None, "year")),
        check_vma=False,
    )
```

```python
import jax
import jax.numpy as jnp
import numpy as np
from jax import lax
from jax.experimental import pallas as pl
from jax.experimental.pallas import tpu as pltpu
from jax.sharding import PartitionSpec as P

HALF = 30
LANE = 128
CHUNKS = 2
MIB = 1024 * 1024
FIRST_LIMIT = 12
NEXT_LIMIT = 12


def vmem():
    return pl.BlockSpec(memory_space=pltpu.VMEM)


def smem():
    return pl.BlockSpec(memory_space=pltpu.SMEM)


def anywhere():
    return pl.BlockSpec(memory_space=pltpu.HBM)


def position(place, stream, shares):
    share, parity = place[1], place[2]
    rising = parity == stream
    return jnp.where(rising, share, shares - 1 - share), rising


def shapes(cells, shares):
    tiles = cells // LANE
    part = cells // shares
    firsts = [share * part // LANE for share in range(shares)]
    size = max(-(-(share + 1) * part // LANE) - firsts[share] for share in range(shares))
    firsts = [min(first, tiles - size) * LANE for first in firsts]
    sizes = [(size + index) // CHUNKS * LANE for index in range(CHUNKS)]
    offsets = [sum(sizes[:index]) for index in range(CHUNKS)]
    return firsts, offsets, sizes


def two_terms(value):
    high = value.astype(jnp.bfloat16)
    rest = value - high.astype(jnp.float32)
    return high, rest.astype(jnp.bfloat16)


def times(left, right):
    return jnp.dot(left, right, preferred_element_type=jnp.float32)


def iota(shape, axis):
    return lax.broadcasted_iota(jnp.int32, shape, axis)


def selector_of(table, hours, day_dev, tall):
    kinds = hours + 1
    year_dev = table.shape[0] // kinds
    rows, slots = (day_dev + 1) * hours, year_dev * day_dev * hours
    per_year = day_dev * hours
    column, row = (0, 1) if tall else (1, 0)

    def pieces(shape, axis, size):
        index = iota(shape, axis)
        quotient = jnp.zeros(shape, jnp.int32)
        for step in range(1, -(-shape[axis] // size)):
            quotient += (index >= step * size).astype(jnp.int32)
        return quotient, index - quotient * size

    def turned(shape):
        return shape[::-1] if tall else shape

    year, within = pieces(turned((1, slots)), column, per_year)
    slot, hour = pieces_of(within, hours)
    spread_slot = iota(turned((day_dev, slots)), row)
    spread = (spread_slot == slot).astype(jnp.float32)
    if tall:
        product = lax.dot_general(
            spread, table, (((1,), (1,)), ((), ())), preferred_element_type=jnp.float32
        )
    else:
        product = times(table, spread)
    kind = iota(turned((table.shape[0], slots)), row)
    moved = jnp.sum(jnp.where(kind == year * kinds, product, 0.0), axis=row, keepdims=True)
    counts = jnp.sum(
        jnp.where(kind == year * kinds + 1 + hour, product, 0.0), axis=row, keepdims=True
    )
    day, row_hour = pieces_of(iota(turned((rows, 1)), row), hours)
    matched = (day == slot + moved.astype(jnp.int32)) & (row_hour == hour)
    return matched, counts


def pieces_of(index, hours):
    quotient = lax.div(index, jnp.int32(hours))
    return quotient, index - quotient * hours


def partial_sums(field, table, picks, lows, width, first, limit):
    year_dev, day_dev, hours, _ = field.shape
    rows, slots = (day_dev + 1) * hours, year_dev * day_dev * hours
    shares = len(lows)
    full = width + (LANE if first else 0)
    order = [shares - 1, *range(shares - 1)]

    def kernel(field_ref, given_ref, out_ref, held, *refs):
        sems = refs[-1]

        def copy(share):
            return pltpu.make_async_copy(
                field_ref.at[:, :, :, pl.ds(lows[share], width)], held.at[share], sems.at[share]
            )

        for share in order:
            copy(share).start()
        if first:
            matched, counts = selector_of(given_ref[...], hours, day_dev, False)
            chosen = jnp.where(matched, counts, 0.0).astype(jnp.bfloat16)
            refs[0][...] = chosen
            tall, _ = selector_of(given_ref[...], hours, day_dev, True)
            refs[1][...] = tall.astype(jnp.bfloat16)
            counts = times(chosen, jnp.ones((slots, LANE), jnp.bfloat16))
        else:
            chosen = given_ref[...]
        for share in order:
            copy(share).wait()
            out_ref[share, :, :width] = times(chosen, held[share].reshape(slots, width))
            if first:
                out_ref[share, :, width:] = counts

    outs = [
        jax.ShapeDtypeStruct((shares, rows, full), jnp.float32),
        jax.ShapeDtypeStruct((shares, year_dev, day_dev, hours, width), jnp.bfloat16),
    ]
    if first:
        outs += [
            jax.ShapeDtypeStruct((rows, slots), jnp.bfloat16),
            jax.ShapeDtypeStruct((slots, rows), jnp.bfloat16),
        ]
    return pl.pallas_call(
        kernel,
        in_specs=[anywhere(), vmem()],
        out_specs=[vmem()] * len(outs),
        out_shape=outs,
        scratch_shapes=[pltpu.SemaphoreType.DMA((shares,))],
        compiler_params=pltpu.CompilerParams(vmem_limit_bytes=limit * MIB),
        cost_estimate=pl.CostEstimate(
            flops=2 * rows * slots * full * shares,
            bytes_accessed=2 * slots * width * shares,
            transcendentals=0,
        ),
        name="partial_sums",
    )(field, table if first else picks)


def mixed(place, partial, received, stream, step):
    shares, rows, full = partial.shape

    def kernel(place_ref, partial_ref, *refs):
        where, rising = position(place_ref, stream, shares)
        ahead = jnp.minimum(shares - step + where, shares - 1)
        value = partial_ref[jnp.where(rising, ahead, shares - 1 - ahead)]
        if received is not None:
            value += jnp.where(where > 0, refs[0][...], 0.0)
        refs[-1][...] = value

    operands = [place, partial] + ([] if received is None else [received])
    return pl.pallas_call(
        kernel,
        in_specs=[smem()] + [vmem()] * (len(operands) - 1),
        out_specs=vmem(),
        out_shape=jax.ShapeDtypeStruct((rows, full), jnp.float32),
        compiler_params=pltpu.CompilerParams(vmem_limit_bytes=4 * MIB),
        cost_estimate=pl.CostEstimate(
            flops=2 * rows * full, bytes_accessed=12 * rows * full, transcendentals=0
        ),
        name="mixed",
    )(*operands)


def totalled(place, partial, received, cuts):
    shares, rows, full = partial.shape
    amount = len(received)

    def kernel(place_ref, partial_ref, *refs):
        value = partial_ref[place_ref[1]]
        for stream in range(amount):
            where, _ = position(place_ref, stream, shares)
            value += jnp.where(where > 0, refs[stream][...], 0.0)
        for out_ref, (low, high) in zip(refs[amount:], cuts):
            out_ref[...] = value[low:high]

    return pl.pallas_call(
        kernel,
        in_specs=[smem()] + [vmem()] * (amount + 1),
        out_specs=[vmem()] * len(cuts),
        out_shape=[jax.ShapeDtypeStruct((high - low, full), jnp.float32) for low, high in cuts],
        compiler_params=pltpu.CompilerParams(vmem_limit_bytes=4 * MIB),
        cost_estimate=pl.CostEstimate(
            flops=2 * rows * full, bytes_accessed=16 * rows * full, transcendentals=0
        ),
        name="totalled",
    )(place, partial, *received)


def smoothed(pieces, band, counts, width):
    rows = band.shape[0]
    full = pieces[0].shape[1]
    with_counts = counts is None
    amount = len(pieces)

    def kernel(*refs):
        piece_refs, band_ref, rest = refs[:amount], refs[amount], refs[amount + 1 :]
        terms = [two_terms(piece_ref[...]) for piece_ref in piece_refs]
        band = band_ref[...]
        total = times(band, jnp.concatenate([term[0] for term in terms], axis=0))
        total += times(band, jnp.concatenate([term[1] for term in terms], axis=0))
        if with_counts:
            rest[1][...] = total[:, width:]
            rest[0][...] = total[:, :width] / total[:, width : width + 1]
        else:
            rest[1][...] = total / rest[0][:, :1]

    out_shape = jax.ShapeDtypeStruct((rows, width), jnp.float32)
    operands = list(pieces) + [band]
    out_specs = vmem()
    if with_counts:
        out_shape = (out_shape, jax.ShapeDtypeStruct((rows, LANE), jnp.float32))
        out_specs = (vmem(), vmem())
    else:
        operands.append(counts)
    return pl.pallas_call(
        kernel,
        in_specs=[vmem()] * len(operands),
        out_specs=out_specs,
        out_shape=out_shape,
        compiler_params=pltpu.CompilerParams(vmem_limit_bytes=8 * MIB),
        cost_estimate=pl.CostEstimate(
            flops=8 * rows * rows * full, bytes_accessed=16 * rows * full, transcendentals=0
        ),
        name="smoothed",
    )(*operands)


def anomalies(slots, picker, place, pieces, origins, lows, shape, previous):
    shares, year_dev, day_dev, hours, width = slots.shape
    amount = len(pieces)
    columns, rows = picker.shape

    def kernel(place_ref, slots_ref, picker_ref, *refs):
        piece_refs = refs[:amount]
        refs = refs[amount:]
        if previous is not None:
            refs = refs[1:]
        out_ref, made, sems = refs

        def source(index):
            stream, step = origins[index]
            _, rising = position(place_ref, stream, shares)
            return place_ref[1] + jnp.where(rising, -step, step)

        def store(index):
            origin = source(index)
            first = jnp.int32(lows[0] // LANE)
            for share in range(1, shares):
                first = jnp.where(origin == share, lows[share] // LANE, first)
            lane = pl.ds(pl.multiple_of(first * LANE, LANE), width)
            return pltpu.make_async_copy(
                made.at[index], out_ref.at[:, :, :, lane], sems.at[index]
            )

        def when_taken(index):
            origin = source(index)
            return pl.when((origin >= 0) & (origin < shares))

        for index in range(amount):
            @when_taken(index)
            def _():
                climate = piece_refs[index][...]
                high = climate.astype(jnp.bfloat16)
                rest = climate - high.astype(jnp.float32)
                middle = rest.astype(jnp.bfloat16)
                low = (rest - middle.astype(jnp.float32)).astype(jnp.bfloat16)
                pick = picker_ref[...]
                expected = times(pick, high) + (times(pick, middle) + times(pick, low))
                values = slots_ref[source(index)].reshape(columns, width).astype(jnp.float32)
                result = (values - expected).astype(jnp.bfloat16)
                made[index] = result.reshape(year_dev, day_dev, hours, width)
                store(index).start()

        for index in range(amount):
            when_taken(index)(lambda: store(index).wait())

    operands = [place, slots, picker] + list(pieces)
    specs = [smem(), vmem(), vmem()] + [vmem()] * amount
    aliases = {}
    if previous is not None:
        aliases = {len(operands): 0}
        operands.append(previous)
        specs.append(anywhere())
    return pl.pallas_call(
        kernel,
        in_specs=specs,
        out_specs=anywhere(),
        out_shape=jax.ShapeDtypeStruct(shape, jnp.bfloat16),
        scratch_shapes=[
            pltpu.VMEM((amount, year_dev, day_dev, hours, width), jnp.bfloat16),
            pltpu.SemaphoreType.DMA((amount,)),
        ],
        input_output_aliases=aliases,
        compiler_params=pltpu.CompilerParams(vmem_limit_bytes=8 * MIB),
        cost_estimate=pl.CostEstimate(
            flops=6 * rows * columns * width * amount,
            bytes_accessed=4 * columns * width * amount,
            transcendentals=0,
        ),
        name="anomalies",
    )(*operands)


def lanes(days, shares, turn):
    pairs = []
    for day in range(days):
        for share in range(shares):
            ahead = share + (1 if day % 2 == turn else -1)
            if 0 <= ahead < shares:
                pairs.append((day * shares + share, day * shares + ahead))
            elif (day ^ 1) < days:
                pairs.append((day * shares + share, (day ^ 1) * shares + share))
    return pairs


def neighbours(day_dev):
    reach = -(-(HALF + day_dev) // day_dev)
    found = []
    for distance in range(-reach, reach + 1):
        kept = [
            row
            for row in range(day_dev + 1)
            if any(abs(distance * day_dev + row - own) <= HALF for own in range(day_dev + 1))
        ]
        if kept:
            found.append((distance, kept[0], kept[-1] + 1))
    return sorted(found, key=lambda entry: -abs(entry[0]))


def band_of(blocks, day_dev, hours):
    target = np.arange((day_dev + 1) * hours)
    columns = []
    for distance, low, high in blocks:
        source = np.arange(low * hours, high * hours)
        apart = distance * day_dev + source[None] // hours - target[:, None] // hours
        same = source[None] % hours == target[:, None] % hours
        columns.append(same & (np.abs(apart) <= HALF))
    return jnp.asarray(np.concatenate(columns, axis=1), jnp.bfloat16)


def local(field, day_index, sample_count):
    year_dev, day_dev, hours, cells = field.shape
    days = lax.axis_size("day")
    shares = lax.axis_size("year")
    day = lax.axis_index("day")
    share = lax.axis_index("year")
    parity = lax.rem(day, 2)
    firsts, offsets, sizes = shapes(cells, shares)
    hops = [lanes(days, shares, turn) for turn in range(2)]

    def send(value, pairs, axes=("day", "year")):
        return lax.ppermute(value, axes, pairs)

    place = jnp.stack([day * day_dev, share, parity]).astype(jnp.int32)
    expected = day * day_dev + iota((year_dev, 1, day_dev), 2)
    moved = (day_index[:, None, :] != expected).astype(jnp.int32)
    table = jnp.concatenate([moved, jnp.transpose(sample_count, (0, 2, 1))], axis=1)
    table = table.reshape(year_dev * (hours + 1), day_dev).astype(jnp.float32)
    partials, slots = [], []
    selector = picker = None
    for k in range(CHUNKS):
        lows = [first + offsets[k] for first in firsts]
        made = partial_sums(
            field, table, selector, lows, sizes[k], k == 0, FIRST_LIMIT if k == 0 else NEXT_LIMIT
        )
        partials.append(made[0])
        slots.append(made[1])
        if k == 0:
            selector, picker = made[2:]

    received = [[None, None] for _ in range(CHUNKS)]
    for step in range(1, shares):
        for k in range(CHUNKS):
            for s in range(2):
                value = mixed(place, partials[k], received[k][s], s, step)
                received[k][s] = send(value, hops[s])

    blocks = neighbours(day_dev)
    band = band_of(blocks, day_dev, hours)
    climates, window_counts = [], None
    for k in range(CHUNKS):
        cuts = sorted({(low * hours, high * hours) for _, low, high in blocks})
        arrived = [value for value in received[k] if value is not None]
        parts = dict(zip(cuts, totalled(place, partials[k], arrived, cuts)))
        pieces = []
        for distance, low, high in blocks:
            piece = parts[low * hours, high * hours]
            if distance:
                pairs = [(source, (source - distance) % days) for source in range(days)]
                piece = send(piece, pairs, "day")
            pieces.append(piece)
        if k == 0:
            climate, window_counts = smoothed(pieces, band, None, sizes[k])
        else:
            climate = smoothed(pieces, band, window_counts, sizes[k])
        climates.append(climate)

    part = cells // shares
    inside = share * part - jnp.asarray(firsts, jnp.int32)[share]
    mine = jnp.concatenate(climates, axis=1).astype(jnp.bfloat16)
    mine = lax.dynamic_slice_in_dim(mine, inside, part, 1)
    mine = mine.reshape(day_dev + 1, hours, part)[:day_dev]

    gathered = [[[], []] for _ in range(CHUNKS)]
    for _ in range(1, shares):
        for k in range(CHUNKS):
            for s in range(2):
                value = gathered[k][s][-1] if gathered[k][s] else climates[k]
                gathered[k][s].append(send(value, hops[s]))

    anomaly = None
    for step in range(shares):
        for k in range(CHUNKS):
            lows = [first + offsets[k] for first in firsts]
            origins = [(s, step) for s in range(2 if step else 1)]
            parts = [gathered[k][s][step - 1] if step else climates[k] for s, _ in origins]
            anomaly = anomalies(slots[k], picker, place, parts, origins, lows, field.shape, anomaly)
    return anomaly, mine


def solution(mesh):
    return jax.shard_map(
        local,
        mesh=mesh,
        in_specs=(P("year", "day", None, None), P("year", "day"), P("year", "day", None)),
        out_specs=(P("year", "day", None, None), P("day", None, "year")),
        check_vma=False,
    )
```
